32 devices in a mesh: ctx: 16 (over z, x, core), fsdp: 2 (over y).
Axes of the slice: x: 2, y: 2, z: 4, core: 2. Of those that a mesh axis runs over, the one named last changes fastest.
Arguments:
- layer_input: bfloat16 [2048, 4096], P('ctx'), may hold values from -8 to 8
- gain: float32 [4096], replicated, may hold values from 0.5 to 1.5
- codes: int32 [4096, 384], P('fsdp'), may hold values from -2147483648 to 2147483646
- column_scale_quantized: int32 [64, 3072], P('fsdp'), may hold values from 0 to 255
- block_second_scale: float32 [64], replicated, may hold values from 0.03 to 0.12
- query_down_map: bfloat16 [4096, 16], replicated, may hold values from -0.09375 to 0.09375
- query_up_map: bfloat16 [16, 2048], P(None, 'fsdp'), may hold values from -0.29882812 to 0.29882812
- token_document: int32 [2048], P('ctx'), may hold values from 0 to 3, as said below
- output_cotangent: bfloat16 [2048, 2048], P('ctx', 'fsdp'), may hold values from -0.059814453 to 0.059814453
Outputs:
- attn: bfloat16 [2048, 2048], P('ctx', 'fsdp')
- grad_a: float32 [4096, 16], replicated
- up_map_gradient: float32 [16, 2048], P(None, 'fsdp')
The draws below stay inside these ranges and needn't reach their ends.
Inputs may be any that keep to these rules, and one draw needn't show every extreme that they name: token_document never falls along the sequence; each document has 1 to 1536 tokens and one has exactly 1536.
All inputs are finite; a program needn't handle non-finite values.
Results may differ from the reference program's by a relative error of at most 0.028.
Values may be sent and summed in bfloat16 or wider, within the bound.
No kernel may reach another device: no remote copies, remote signals or barrier semaphores. Data moves between devices by JAX's collectives and lax.ppermute only.
A program may use at most 192 MiB of HBM per device.

```python
import math
import jax
import jax.numpy as jnp
import numpy as np
from jax import lax

MODEL_WIDTH = 4096
QUERY_HEADS = 16
KEY_VALUE_HEADS = 4
HEAD_SIZE = 128
ADAPTER_RANK = 16
DOCS = 4
SEQUENCE_TOKENS = 2048
MOST = 1536
QUERY_FEATURES = 2048
COLS = 3072
N_FSDP = 2


NF4_LEVELS = [-1.0, -0.6961928009986877, -0.5250730514526367, -0.39491748809814453, -0.28444138169288635, -0.18477343022823334, -0.09105003625154495, 0.0, 0.07958029955625534, 0.16093020141124725, 0.24611230194568634, 0.33791524171829224, 0.44070982933044434, 0.5626170039176941, 0.7229568362236023, 1.0]


def weight_parts(key):
    code_key = jax.random.fold_in(key, 101)
    scale_key = jax.random.fold_in(key, 102)
    const_key = jax.random.fold_in(key, 103)
    packed = jax.random.randint(code_key, (MODEL_WIDTH, COLS // 8), -2147483648, 2147483647, dtype=jnp.int32)
    scales = jax.random.randint(scale_key, (MODEL_WIDTH // 64, COLS), 0, 256, dtype=jnp.int32)
    lower, upper = (0.03, 0.09)
    consts = jnp.exp(jax.random.uniform(const_key, (MODEL_WIDTH // 64,), jnp.float32, math.log(lower), math.log(upper)))
    return (packed, scales, consts)


def unpack_weights(packed, scales, consts):
    row_count = packed.shape[0]
    pieces = [jnp.bitwise_and(jnp.right_shift(packed, 4 * nibble), 15) for nibble in range(8)]
    unpacked = jnp.stack(pieces, axis=-1).reshape(row_count, packed.shape[1] * 8)
    table = jnp.asarray(NF4_LEVELS, jnp.float32)
    levels = table[unpacked]
    absmax = (scales.astype(jnp.float32) + 1.0) / 256.0 * consts[:, None]
    return (levels.reshape(row_count // 64, 64, -1) * absmax[:, None, :]).reshape(row_count, -1)


def doc_layout(key):
    layout_key = jax.random.fold_in(key, 401)
    long_slot = jax.random.randint(jax.random.fold_in(layout_key, 1), (), 1, DOCS, dtype=jnp.int32)
    remaining = jnp.int32(SEQUENCE_TOKENS - MOST)
    others = []
    for number in range(DOCS - 2):
        upper_len = remaining - (DOCS - 2 - number) + 1
        length_now = jax.random.randint(jax.random.fold_in(layout_key, 10 + number), (), 1, upper_len, dtype=jnp.int32)
        others.append(length_now)
        remaining = remaining - length_now
    others.append(remaining)
    lengths = []
    for number in range(DOCS):
        before = others[min(number, DOCS - 2)]
        after = others[max(number - 1, 0)]
        lengths.append(jnp.where(number < long_slot, before, jnp.where(number == long_slot, jnp.int32(MOST), after)))
    lengths = jnp.stack(lengths).astype(jnp.int32)
    ends = jnp.cumsum(lengths).astype(jnp.int32)
    positions = jnp.arange(SEQUENCE_TOKENS, dtype=jnp.int32)
    ids = jnp.sum((positions[:, None] >= ends[None, :DOCS - 1]).astype(jnp.int32), axis=1).astype(jnp.int32)
    starts = ends - lengths
    long_start = jnp.sum(jnp.where(jnp.arange(DOCS, dtype=jnp.int32) == long_slot, starts, 0)).astype(jnp.int32)
    return (ids, long_start)


def draw_token_document(key, part):
    return doc_layout(key)[0]


def draw_codes(key, part):
    return weight_parts(key)[0]


def draw_column_scale_quantized(key, part):
    return weight_parts(key)[1]


def draw_block_second_scale(key, part):
    return weight_parts(key)[2]


def far_pairs(key, fields, weight):
    long_start = doc_layout(key)[1]
    hq_local = QUERY_HEADS // N_FSDP
    key_value_local = KEY_VALUE_HEADS // N_FSDP
    group_columns = COLS // N_FSDP
    head_grouped = QUERY_HEADS // KEY_VALUE_HEADS
    half_size = HEAD_SIZE // 2
    edge_dims = max(HEAD_SIZE // 16, 1)
    aligned = list(range(half_size - edge_dims, half_size)) + list(range(HEAD_SIZE - edge_dims, HEAD_SIZE))
    root_width = math.sqrt(MODEL_WIDTH)
    for plant in range(8):
        query_head = 3 * plant % QUERY_HEADS
        group_id = query_head // hq_local
        key_head = query_head // head_grouped
        query_cols = np.array([group_id * group_columns + (query_head - group_id * hq_local) * HEAD_SIZE + dim for dim in aligned])
        key_cols = np.array([group_id * group_columns + hq_local * HEAD_SIZE + (key_head - group_id * key_value_local) * HEAD_SIZE + dim for dim in aligned])
        columns = jnp.concatenate([weight[:, query_cols], weight[:, key_cols]], axis=1)
        direction = jnp.sum(columns, axis=1)
        direction = direction / jnp.sqrt(jnp.sum(direction * direction))
        offset = jax.random.randint(jax.random.fold_in(key, 500 + plant), (), 0, SEQUENCE_TOKENS // 4, dtype=jnp.int32)
        position = long_start + offset
        vector = root_width * direction
        fields = fields.at[position].set(vector)
        fields = fields.at[position + SEQUENCE_TOKENS // 2].set(vector)
    return fields


def draw_layer_input(key, part):
    fields = jax.random.normal(jax.random.fold_in(key, 201), (SEQUENCE_TOKENS, MODEL_WIDTH), jnp.float32)
    packed, scales, consts = weight_parts(key)
    weight = unpack_weights(packed, scales, consts)
    fields = far_pairs(key, fields, weight)
    return jnp.clip(fields, -6.0, 6.0).astype(jnp.bfloat16)


def shard_levels(stream_key, shape, shards, low, top_value):
    level = 1.0
    for dim, shards_of in shards:
        steps = jax.random.uniform(jax.random.fold_in(jax.random.fold_in(stream_key, 6), dim), (shards_of,), jnp.float32, low / len(shards), top_value / len(shards))
        level = level * jnp.repeat(jnp.exp(steps), shape[dim] // shards_of).reshape((-1,) + (1,) * (len(shape) - 1 - dim))
    return level


def bell_draw(key, dims, width, most, cuts=(), held_as=jnp.bfloat16):
    result = jax.random.normal(key, dims, jnp.float32) * width
    if len(cuts) > 0:
        result = shard_levels(key, dims, cuts, -0.22, 0.18) * result
    return jnp.clip(result, min=-most, max=most).astype(held_as)


def setup_inputs(seed: int = 0) -> dict:
    splits = jax.random.split(jax.random.key(seed), 10)
    layer_input = draw_layer_input(jax.random.fold_in(splits[9], 71), 0)
    gain = jnp.clip(1.0 + 0.1 * jax.random.normal(splits[1], (MODEL_WIDTH,), jnp.float32), 0.5, 1.5)
    codes = draw_codes(jax.random.fold_in(splits[9], 71), 0)
    column_scale_quantized = draw_column_scale_quantized(jax.random.fold_in(splits[9], 71), 0)
    block_second_scale = draw_block_second_scale(jax.random.fold_in(splits[9], 71), 0)
    query_down_map = bell_draw(splits[5], (MODEL_WIDTH, ADAPTER_RANK), MODEL_WIDTH ** -0.5, 0.09375)
    query_up_map = bell_draw(splits[6], (ADAPTER_RANK, QUERY_FEATURES), 0.05, 0.29882812, ((1, 2),))
    token_document = draw_token_document(jax.random.fold_in(splits[9], 71), 0)
    output_cotangent = bell_draw(splits[8], (SEQUENCE_TOKENS, QUERY_FEATURES), 0.01, 0.059814453, ((0, 16), (1, 2)))
    return {"layer_input": layer_input, "gain": gain, "codes": codes, "column_scale_quantized": column_scale_quantized, "block_second_scale": block_second_scale, "query_down_map": query_down_map, "query_up_map": query_up_map, "token_document": token_document, "output_cotangent": output_cotangent}


NF4_LEVELS = [-1.0, -0.6961928009986877, -0.5250730514526367, -0.39491748809814453, -0.28444138169288635, -0.18477343022823334, -0.09105003625154495, 0.0, 0.07958029955625534, 0.16093020141124725, 0.24611230194568634, 0.33791524171829224, 0.44070982933044434, 0.5626170039176941, 0.7229568362236023, 1.0]
ADAPTER_SCALE = 2.0
ROPE_BASE = 500000.0

def dequantize(packed, column_scale_quantized, block_second_scale):
    row_count = packed.shape[0]
    pieces = [jnp.bitwise_and(jnp.right_shift(packed, 4 * nibble), 15) for nibble in range(8)]
    unpacked = jnp.stack(pieces, axis=-1).reshape(row_count, packed.shape[1] * 8)
    levels = jnp.zeros(unpacked.shape, jnp.float32)
    for slot_code, level_value in enumerate(NF4_LEVELS):
        levels = levels + jnp.where(unpacked == slot_code, jnp.float32(level_value), jnp.float32(0.0))
    absmax = (column_scale_quantized.astype(jnp.float32) + 1.0) / 256.0 * block_second_scale[:, None]
    scaled = levels.reshape(row_count // 64, 64, -1) * absmax[:, None, :]
    return scaled.reshape(row_count, -1).astype(jnp.bfloat16)

def rope_angles(positions):
    freqs = jnp.exp(jnp.arange(HEAD_SIZE // 2, dtype=jnp.float32) * (-2.0 * math.log(ROPE_BASE) / HEAD_SIZE))
    angle = positions.astype(jnp.float32)[:, None] * freqs[None, :]
    cosine = jnp.concatenate([jnp.cos(angle), jnp.cos(angle)], axis=-1)
    sine = jnp.concatenate([jnp.sin(angle), jnp.sin(angle)], axis=-1)
    return (cosine, sine)

def apply_rotation(field, rotary_phases):
    cosine, sine = rotary_phases
    half = HEAD_SIZE // 2
    turned = jnp.concatenate([-field[..., half:], field[..., :half]], axis=-1)
    return field * cosine[:, None, :] + turned * sine[:, None, :]

def rotate_back(grads, rotary_phases):
    cosine, sine = rotary_phases
    half = HEAD_SIZE // 2
    scaled = grads * sine[:, None, :]
    turned = jnp.concatenate([-scaled[..., half:], scaled[..., :half]], axis=-1)
    return grads * cosine[:, None, :] - turned

def rms_norm(layer_input, gain):
    wide = layer_input.astype(jnp.float32)
    inverse = lax.rsqrt(lax.optimization_barrier(jnp.mean(wide * wide, axis=-1, keepdims=True)) + 1e-05)
    return (wide * inverse * gain[None, :]).astype(jnp.bfloat16)

def reference(layer_input, gain, codes, column_scale_quantized, block_second_scale, query_down_map, query_up_map, token_document, output_cotangent):
    input_normalized = rms_norm(layer_input, gain)
    weight = dequantize(codes, column_scale_quantized, block_second_scale)
    projection_output = jnp.dot(input_normalized.astype(jnp.float32), weight.astype(jnp.float32), preferred_element_type=jnp.float32)
    group_columns = (QUERY_HEADS + 2 * KEY_VALUE_HEADS) * HEAD_SIZE // N_FSDP
    q_local = QUERY_HEADS // N_FSDP * HEAD_SIZE
    key_value_local = KEY_VALUE_HEADS // N_FSDP * HEAD_SIZE
    query_slices, key_slices, value_slices = ([], [], [])
    for member in range(N_FSDP):
        anchor = member * group_columns
        query_slices.append(projection_output[:, anchor:anchor + q_local])
        key_slices.append(projection_output[:, anchor + q_local:anchor + q_local + key_value_local])
        value_slices.append(projection_output[:, anchor + q_local + key_value_local:anchor + group_columns])
    rank_reduced = jnp.dot(input_normalized.astype(jnp.float32), query_down_map.astype(jnp.float32), preferred_element_type=jnp.float32).astype(jnp.bfloat16)
    query_complete = jnp.concatenate(query_slices, axis=1) + ADAPTER_SCALE * jnp.dot(rank_reduced.astype(jnp.float32), query_up_map.astype(jnp.float32), preferred_element_type=jnp.float32)
    positions = jnp.arange(SEQUENCE_TOKENS, dtype=jnp.int32)
    rotary_phases = rope_angles(positions)
    query_rows = apply_rotation(query_complete.reshape(SEQUENCE_TOKENS, QUERY_HEADS, HEAD_SIZE), rotary_phases).astype(jnp.bfloat16)
    key_rows = apply_rotation(jnp.concatenate(key_slices, axis=1).reshape(SEQUENCE_TOKENS, KEY_VALUE_HEADS, HEAD_SIZE), rotary_phases).astype(jnp.bfloat16)
    value_rows = jnp.concatenate(value_slices, axis=1).reshape(SEQUENCE_TOKENS, KEY_VALUE_HEADS, HEAD_SIZE).astype(jnp.bfloat16)
    head_grouped = QUERY_HEADS // KEY_VALUE_HEADS
    query_grouped = query_rows.reshape(SEQUENCE_TOKENS, KEY_VALUE_HEADS, head_grouped, HEAD_SIZE).astype(jnp.float32)
    grouped_gradient = output_cotangent.reshape(SEQUENCE_TOKENS, KEY_VALUE_HEADS, head_grouped, HEAD_SIZE).astype(jnp.float32)
    keys_wide = key_rows.astype(jnp.float32)
    values_wide = value_rows.astype(jnp.float32)
    soft_scale = 1.0 / math.sqrt(HEAD_SIZE)
    block = math.gcd(SEQUENCE_TOKENS, 256)

    def one_block(block_id):
        start = (block_id * block).astype(jnp.int32)
        query_blk = lax.dynamic_slice_in_dim(query_grouped, start, block, 0)
        grad_blk = lax.dynamic_slice_in_dim(grouped_gradient, start, block, 0)
        ids_blk = lax.dynamic_slice_in_dim(token_document, start, block, 0)
        pos_blk = start + jnp.arange(block, dtype=jnp.int32)
        allowed = (ids_blk[:, None] == token_document[None, :]) & (positions[None, :] <= pos_blk[:, None])
        scores = jnp.einsum('bhgd,shd->hgbs', query_blk, keys_wide) * soft_scale
        masked = jnp.where(allowed, scores, -1e+30)
        top = lax.optimization_barrier(jnp.max(masked, axis=-1, keepdims=True))
        expo = jnp.where(allowed, jnp.exp(masked - top), 0.0)
        probs = expo / lax.optimization_barrier(jnp.sum(expo, axis=-1, keepdims=True))
        rounded = probs.astype(jnp.bfloat16).astype(jnp.float32)
        output = jnp.einsum('hgbs,shd->bhgd', rounded, values_wide)
        grad_dots = jnp.einsum('bhgd,shd->hgbs', grad_blk, values_wide)
        mean_dot = lax.optimization_barrier(jnp.sum(probs * grad_dots, axis=-1, keepdims=True))
        grad_scores = (probs * (grad_dots - mean_dot)).astype(jnp.bfloat16).astype(jnp.float32)
        grad_query = jnp.einsum('hgbs,shd->bhgd', grad_scores, keys_wide) * soft_scale
        return (output, grad_query)
    outputs, grad_queries = lax.map(one_block, jnp.arange(SEQUENCE_TOKENS // block, dtype=jnp.int32))
    attn = outputs.reshape(SEQUENCE_TOKENS, QUERY_HEADS * HEAD_SIZE).astype(jnp.bfloat16)
    linear_gradient = rotate_back(grad_queries.reshape(SEQUENCE_TOKENS, QUERY_HEADS, HEAD_SIZE), rotary_phases).reshape(SEQUENCE_TOKENS, QUERY_HEADS * HEAD_SIZE).astype(jnp.bfloat16)
    up_map_gradient = ADAPTER_SCALE * jnp.dot(rank_reduced.T.astype(jnp.float32), linear_gradient.astype(jnp.float32), preferred_element_type=jnp.float32)
    middle_gradient = (ADAPTER_SCALE * jnp.dot(linear_gradient.astype(jnp.float32), query_up_map.T.astype(jnp.float32), preferred_element_type=jnp.float32)).astype(jnp.bfloat16)
    grad_a = jnp.dot(input_normalized.T.astype(jnp.float32), middle_gradient.astype(jnp.float32), preferred_element_type=jnp.float32)
    return (attn, grad_a, up_map_gradient)
```

```python
import functools
import math

import jax
import jax.numpy as jnp
from jax import lax
from jax.experimental import pallas as pl
from jax.experimental.pallas import tpu as pltpu
from jax.sharding import PartitionSpec as P

HEAD_SIZE = 128
BLOCK_ROWS = 64
NIBBLES = 8
GROUP = HEAD_SIZE // NIBBLES
DEPTH = 256

NF4_LEVELS = [
    -1.0,
    -0.6961928009986877,
    -0.5250730514526367,
    -0.39491748809814453,
    -0.28444138169288635,
    -0.18477343022823334,
    -0.09105003625154495,
    0.0,
    0.07958029955625534,
    0.16093020141124725,
    0.24611230194568634,
    0.33791524171829224,
    0.44070982933044434,
    0.5626170039176941,
    0.7229568362236023,
    1.0,
]
ADAPTER_SCALE = 2.0
ROPE_BASE = 500000.0
F32 = jnp.float32
BF16 = jnp.bfloat16


def vmem(count):
    return [pl.BlockSpec(memory_space=pltpu.VMEM)] * count


def nt(a, b):
    return lax.dot_general(a, b, (((1,), (1,)), ((), ())), preferred_element_type=F32)


def tn(a, b):
    return lax.dot_general(a, b, (((0,), (0,)), ((), ())), preferred_element_type=F32)


def nn(a, b):
    return jnp.dot(a, b, preferred_element_type=F32)


def feature_permutation():
    place = lax.broadcasted_iota(jnp.int32, (HEAD_SIZE, HEAD_SIZE), 0)
    feature = lax.broadcasted_iota(jnp.int32, (HEAD_SIZE, HEAD_SIZE), 1)
    hit = feature == NIBBLES * (place % GROUP) + place // GROUP
    return jnp.where(hit, 1.0, 0.0).astype(BF16)


def spread_scales(scale_ref, second_ref, member, sub_tiles, out_ref):
    blocks = scale_ref.shape[0]
    width = second_ref.shape[1]
    row = lax.broadcasted_iota(jnp.int32, (blocks, width), 0) + member * blocks
    lane = lax.broadcasted_iota(jnp.int32, (blocks, width), 1)
    second = jnp.sum(jnp.where(row == lane, second_ref[...], 0.0), axis=1, keepdims=True)
    order = feature_permutation()
    turned = []
    for tile in sub_tiles:
        if isinstance(tile, int):
            codes = scale_ref[:, tile * HEAD_SIZE : (tile + 1) * HEAD_SIZE]
        else:
            codes = scale_ref[:, pl.ds(pl.multiple_of(tile * HEAD_SIZE, HEAD_SIZE), HEAD_SIZE)]
        absmax = (codes.astype(F32) + 1.0) / 256.0 * second
        turned.append(nt(order, absmax.astype(BF16)))
    for n in range(NIBBLES):
        column = jnp.concatenate([t[n * GROUP : (n + 1) * GROUP] for t in turned], axis=0)
        out_ref[n] = column.T


def project(words, x_ref, x_start, scales_ref, weight_ref, total_ref, row_count):
    steps = row_count // DEPTH

    def fill(step, slot):
        for part in range(DEPTH // BLOCK_ROWS):
            start = pl.multiple_of(step * DEPTH + part * BLOCK_ROWS, BLOCK_ROWS)
            word = words(start)
            block = step * (DEPTH // BLOCK_ROWS) + part
            for half in range(2):
                code = (lax.shift_right_logical(word, 16) if half else word).astype(jnp.int16)
                for quarter in range(4):
                    n = half * 4 + quarter
                    bits = []
                    for b in range(4):
                        place = 4 * quarter + b
                        if place == 15:
                            bits.append(code < jnp.int16(0))
                        else:
                            bits.append((code & jnp.int16(1 << place)) != jnp.int16(0))
                    level = [
                        jnp.where(bits[3], BF16(NF4_LEVELS[8 + j]), BF16(NF4_LEVELS[j]))
                        for j in range(8)
                    ]
                    level = [jnp.where(bits[2], level[4 + j], level[j]) for j in range(4)]
                    level = [jnp.where(bits[1], level[2 + j], level[j]) for j in range(2)]
                    level = jnp.where(bits[0], level[1], level[0])
                    scale = scales_ref[n, pl.ds(block, 1), :].astype(BF16)
                    weight_ref[
                        slot,
                        part * BLOCK_ROWS : (part + 1) * BLOCK_ROWS,
                        n * HEAD_SIZE : (n + 1) * HEAD_SIZE,
                    ] = level * scale

    def multiply(step, slot):
        start = pl.multiple_of(x_start + step * DEPTH, DEPTH)
        total_ref[...] += nn(x_ref[:, pl.ds(start, DEPTH)], weight_ref[slot])

    total_ref[...] = jnp.zeros_like(total_ref)
    fill(0, 0)

    def body(step, carry):
        multiply(step - 1, (step - 1) % 2)
        fill(step, step % 2)
        return carry

    lax.fori_loop(1, steps, body, 0)
    multiply(steps - 1, (steps - 1) % 2)


def key_value_kernel(
    x_ref,
    gain_ref,
    low_codes_ref,
    high_codes_ref,
    scale_ref,
    second_ref,
    down_ref,
    normed_ref,
    low_rank_ref,
    own_ref,
    send_ref,
    scales_ref,
    weight_ref,
    total_ref,
    turned_ref,
):
    member = lax.axis_index("fsdp")
    row_count = low_codes_ref.shape[0]
    wide = x_ref[...].astype(F32)
    inverse = lax.rsqrt(jnp.mean(wide * wide, axis=-1, keepdims=True) + 1e-05)
    normed_ref[...] = (wide * inverse * gain_ref[...]).astype(BF16)
    low_rank_ref[...] = nt(normed_ref[...], down_ref[...]).astype(BF16)
    spread_scales(scale_ref, second_ref, member, [8, 9, 10, 11, 20, 21, 22, 23], scales_ref)
    lane = lax.broadcasted_iota(jnp.int32, (BLOCK_ROWS, HEAD_SIZE), 1)

    def words(start):
        low = low_codes_ref[pl.ds(start, BLOCK_ROWS), :]
        high = high_codes_ref[pl.ds(start, BLOCK_ROWS), :]
        return jnp.where(lane < HEAD_SIZE // 2, low, high)

    project(words, normed_ref, member * row_count, scales_ref, weight_ref, total_ref, row_count)
    half = HEAD_SIZE // 2
    for n in range(NIBBLES):
        turned_ref[...] = total_ref[:, n * HEAD_SIZE : (n + 1) * HEAD_SIZE].T
        own_ref[n] = turned_ref[pl.ds(pl.multiple_of(member * half, half), half), :]
        other = turned_ref[pl.ds(pl.multiple_of((1 - member) * half, half), half), :]
        send_ref[n] = other.astype(BF16)


def query_kernel(
    first,
    x_ref,
    codes_ref,
    scale_ref,
    second_ref,
    out_ref,
    scales_ref,
    weight_ref,
    total_ref,
):
    member = lax.axis_index("fsdp")
    target = (1 - member) if first else member
    row_count = codes_ref.shape[0]
    tiles = [
        jnp.where(target == 0, k, (16 + k) if k < 4 else (8 + k)) for k in range(NIBBLES)
    ]
    spread_scales(scale_ref, second_ref, member, tiles, scales_ref)
    lane = lax.broadcasted_iota(jnp.int32, (BLOCK_ROWS, HEAD_SIZE), 1)
    is_low = target == 0

    def words(start):
        rows = pl.ds(start, BLOCK_ROWS)
        zero = codes_ref[rows, :HEAD_SIZE]
        low = codes_ref[rows, HEAD_SIZE : 2 * HEAD_SIZE]
        high = codes_ref[rows, 2 * HEAD_SIZE :]
        return jnp.where(is_low, zero, jnp.where(lane < HEAD_SIZE // 2, high, low))

    project(words, x_ref, member * row_count, scales_ref, weight_ref, total_ref, row_count)
    for n in range(NIBBLES):
        out_ref[n] = total_ref[:, n * HEAD_SIZE : (n + 1) * HEAD_SIZE].T.astype(out_ref.dtype)


def rotate_pair(a, b, cosine, sine):
    return a * cosine - b * sine, b * cosine + a * sine


def key_value_finish_kernel(own_ref, got_ref, ids_ref, block_ref, cosine_ref, sine_ref):
    row_count = own_ref.shape[2]
    place = lax.axis_index("ctx")
    half = HEAD_SIZE // 2
    row = lax.broadcasted_iota(jnp.int32, (half, row_count), 0)
    token = lax.broadcasted_iota(jnp.int32, (half, row_count), 1) + place * row_count
    index = NIBBLES * (row % NIBBLES) + row // NIBBLES
    freqs = jnp.exp(index.astype(F32) * (-2.0 * math.log(ROPE_BASE) / HEAD_SIZE))
    angle = token.astype(F32) * freqs
    cosine_ref[...] = jnp.cos(angle)
    sine_ref[...] = jnp.sin(angle)
    order = feature_permutation()
    full = [own_ref[n] + got_ref[n].astype(F32) for n in range(NIBBLES)]
    for head in range(2):
        pieces = []
        for n in range(NIBBLES):
            group = full[n][head * GROUP : (head + 1) * GROUP]
            rows = slice(n * NIBBLES, (n + 1) * NIBBLES)
            pieces.extend(
                rotate_pair(group[:NIBBLES], group[NIBBLES:], cosine_ref[rows], sine_ref[rows])
            )
        keys = jnp.concatenate(pieces, axis=0).T.astype(BF16)
        block_ref[0, head * row_count : (head + 1) * row_count, :] = keys
        values = jnp.concatenate(
            [full[n][(2 + head) * GROUP : (3 + head) * GROUP] for n in range(NIBBLES)], axis=0
        )
        values = nn(values.T.astype(BF16), order).astype(BF16)
        block_ref[0, (2 + head) * row_count : (3 + head) * row_count, :] = values
    ids = jnp.broadcast_to(ids_ref[...].astype(F32), (GROUP, row_count))
    block_ref[0, 4 * row_count :, :] = ids.astype(BF16)


def query_finish_kernel(
    own_ref, got_ref, low_rank_ref, up_ref, cosine_ref, sine_ref, queries_ref, full_ref
):
    member = lax.axis_index("fsdp")
    order = feature_permutation()
    heads = queries_ref.shape[0]
    for n in range(NIBBLES):
        full_ref[n] = own_ref[n] + got_ref[n].astype(F32)
    for head in range(heads):
        up = nt(up_ref[:, head * HEAD_SIZE : (head + 1) * HEAD_SIZE], order).astype(BF16)
        adapter = ADAPTER_SCALE * lax.dot_general(
            up, low_rank_ref[...], (((0,), (1,)), ((), ())), preferred_element_type=F32
        )
        start = pl.multiple_of(((head + member * (heads // 2)) % heads) * GROUP, GROUP)
        pieces = []
        for n in range(NIBBLES):
            group = full_ref[n, pl.ds(start, GROUP), :] + adapter[n * GROUP : (n + 1) * GROUP]
            rows = slice(n * NIBBLES, (n + 1) * NIBBLES)
            pieces.extend(
                rotate_pair(group[:NIBBLES], group[NIBBLES:], cosine_ref[rows], sine_ref[rows])
            )
        queries_ref[head] = jnp.concatenate(pieces, axis=0).T.astype(BF16)


def attention_kernel(
    context,
    queries_ref,
    cotangent_ref,
    own_ref,
    beside_ref,
    core_ref,
    core_beside_ref,
    low_rank_ref,
    normed_ref,
    up_ref,
    cosine_ref,
    sine_ref,
    attn_ref,
    mine_ref,
    other_ref,
    grads_ref,
    top_ref,
    norm_ref,
    dot_ref,
    out_ref,
    grad_ref,
    lin_ref,
):
    place = lax.axis_index("ctx")
    heads, row_count, _ = queries_ref.shape
    grouped = heads // 2
    lists = own_ref.shape[0]
    depth = context.bit_length() - 1
    soft = math.log2(math.e) / math.sqrt(HEAD_SIZE)
    for head in range(heads):
        rows = slice((head % grouped) * row_count, (head % grouped + 1) * row_count)
        grads_ref[head // grouped, rows, :] = cotangent_ref[
            :, head * HEAD_SIZE : (head + 1) * HEAD_SIZE
        ]
    top_ref[...] = jnp.full_like(top_ref, -1e30)
    norm_ref[...] = jnp.zeros_like(norm_ref)
    dot_ref[...] = jnp.zeros_like(dot_ref)
    out_ref[...] = jnp.zeros_like(out_ref)
    grad_ref[...] = jnp.zeros_like(grad_ref)
    square = (row_count, row_count)
    my_ids = own_ref[0, 4 * row_count :, :].astype(F32)[:1]
    row_ids = jnp.broadcast_to(my_ids, square).T
    row_pos = lax.broadcasted_iota(jnp.int32, square, 0) + place * row_count
    lane = lax.broadcasted_iota(jnp.int32, square, 1)
    pieces = (own_ref, beside_ref, core_ref, core_beside_ref)

    def chunk(number, device):
        bias = []
        for piece, flip in zip(pieces, (0, 2, 1, 3)):
            ids = piece[number, 4 * row_count :, :].astype(F32)[:1]
            pos = lane + (device ^ flip) * row_count
            allowed = (row_ids == ids) & (pos <= row_pos)
            bias.append(jnp.where(allowed, 0.0, -1e30))
        bias = jnp.concatenate(bias, axis=1)
        for kv in range(2):
            key_rows = slice(kv * row_count, (kv + 1) * row_count)
            value_rows = slice((2 + kv) * row_count, (3 + kv) * row_count)
            keys = jnp.concatenate([piece[number, key_rows, :] for piece in pieces], axis=0)
            values = jnp.concatenate([piece[number, value_rows, :] for piece in pieces], axis=0)
            both = jnp.concatenate([values, keys], axis=1)
            for g in range(grouped):
                rows = slice(g * row_count, (g + 1) * row_count)
                scores = nt(queries_ref[kv * grouped + g], keys) * soft + bias
                dots = nt(grads_ref[kv, rows, :], values)
                old = top_ref[kv, rows, :]
                new = jnp.maximum(old, jnp.max(scores, axis=1, keepdims=True))
                top_ref[kv, rows, :] = new
                decay = jnp.exp2(old - new)
                expo = jnp.exp2(scores - jnp.concatenate([new] * 4, axis=1))
                weighted = expo * dots
                fold = lambda a: (
                    a[:, :HEAD_SIZE]
                    + a[:, HEAD_SIZE : 2 * HEAD_SIZE]
                    + a[:, 2 * HEAD_SIZE : 3 * HEAD_SIZE]
                    + a[:, 3 * HEAD_SIZE :]
                )
                norm_ref[kv, rows, :] = decay * norm_ref[kv, rows, :] + fold(expo)
                dot_ref[kv, rows, :] = decay * dot_ref[kv, rows, :] + fold(weighted)
                wide = jnp.concatenate([decay, decay], axis=1)
                out_ref[kv, rows, :] = wide * out_ref[kv, rows, :] + nn(expo.astype(BF16), both)
                grad_ref[kv, rows, :] = decay * grad_ref[kv, rows, :] + nn(
                    weighted.astype(BF16), keys
                )

    def body(number, carry):
        flip = 0
        for b in range(depth - 2):
            flip = flip + (((number >> b) & 1) << (depth - 1 - b))
        device = place ^ flip

        @pl.when((device >> 2) <= (place >> 2))
        def _():
            chunk(number, device)

        return carry

    lax.fori_loop(0, lists, body, 0)

    half = HEAD_SIZE // 2
    cosine, sine = [], []
    for n in range(NIBBLES):
        rows = slice(n * NIBBLES, (n + 1) * NIBBLES)
        cosine.extend([cosine_ref[rows]] * 2)
        sine.extend([sine_ref[rows], -sine_ref[rows]])
    cosine = jnp.concatenate(cosine, axis=0).T
    sine = jnp.concatenate(sine, axis=0).T
    low_half = (lax.broadcasted_iota(jnp.int32, square, 1) & NIBBLES) == 0
    order = feature_permutation()
    for head in range(heads):
        kv, g = divmod(head, grouped)
        rows = slice(g * row_count, (g + 1) * row_count)
        columns = slice(head * HEAD_SIZE, (head + 1) * HEAD_SIZE)
        inverse = 1.0 / jnp.sum(norm_ref[kv, rows, :], axis=1, keepdims=True)
        attn_ref[:, columns] = (out_ref[kv, rows, :HEAD_SIZE] * inverse).astype(BF16)
        mean = jnp.sum(dot_ref[kv, rows, :], axis=1, keepdims=True) * inverse
        grad = (grad_ref[kv, rows, :] - mean * out_ref[kv, rows, HEAD_SIZE:]) * (
            inverse * (1.0 / math.sqrt(HEAD_SIZE))
        )
        swapped = jnp.where(
            low_half,
            pltpu.roll(grad, HEAD_SIZE - NIBBLES, 1),
            pltpu.roll(grad, NIBBLES, 1),
        )
        lin = (grad * cosine + swapped * sine).astype(BF16)
        lin_ref[:, columns] = nn(lin, order).astype(BF16)
    middle = (ADAPTER_SCALE * nt(lin_ref[...], up_ref[...])).astype(BF16)
    core = place & 1
    width = normed_ref.shape[1] // 2
    up_width = lin_ref.shape[1] // 2
    mine = pl.ds(pl.multiple_of(core * width, HEAD_SIZE), width)
    other = pl.ds(pl.multiple_of((1 - core) * width, HEAD_SIZE), width)
    mine_ref[:, :width] = tn(middle, normed_ref[:, mine])
    other_ref[:, :width] = tn(middle, normed_ref[:, other]).astype(BF16)
    mine = pl.ds(pl.multiple_of(core * up_width, HEAD_SIZE), up_width)
    other = pl.ds(pl.multiple_of((1 - core) * up_width, HEAD_SIZE), up_width)
    mine_ref[:, width:] = ADAPTER_SCALE * tn(low_rank_ref[...], lin_ref[:, mine])
    other_ref[:, width:] = (ADAPTER_SCALE * tn(low_rank_ref[...], lin_ref[:, other])).astype(BF16)


def cost(flops, size):
    return pl.CostEstimate(flops=int(flops), bytes_accessed=int(size), transcendentals=0)


def on_device(
    context,
    layer_input,
    gain,
    codes,
    column_scale_quantized,
    block_second_scale,
    query_down_map,
    query_up_map,
    token_document,
    output_cotangent,
):
    row_count, width = layer_input.shape
    code_rows, code_width = codes.shape
    rank = query_down_map.shape[1]
    query_width = query_up_map.shape[1]
    heads = query_width // HEAD_SIZE
    half = HEAD_SIZE // 2
    sds = jax.ShapeDtypeStruct

    def flip(array, bit):
        return lax.ppermute(array, "ctx", [(i, i ^ bit) for i in range(context)])

    def swap(array):
        return lax.ppermute(array, "fsdp", [(0, 1), (1, 0)])

    gain_row = gain.reshape(1, width)
    second_row = block_second_scale.reshape(1, -1)
    ids_row = token_document.reshape(1, row_count)
    down_rows = query_down_map.T
    project_scratch = [
        pltpu.VMEM((NIBBLES, code_rows // BLOCK_ROWS, HEAD_SIZE), F32),
        pltpu.VMEM((2, DEPTH, NIBBLES * HEAD_SIZE), BF16),
        pltpu.VMEM((row_count, NIBBLES * HEAD_SIZE), F32),
    ]
    project_cost = cost(1.2e10, code_rows * HEAD_SIZE * 4)
    whole = lambda a: pl.BlockSpec(a.shape, lambda i: (0,) * a.ndim)
    normed, low_rank, kv_own, kv_send = pl.pallas_call(
        key_value_kernel,
        grid=(1,),
        in_specs=[
            whole(layer_input),
            whole(gain_row),
            pl.BlockSpec((code_rows, HEAD_SIZE), lambda i: (0, 1)),
            pl.BlockSpec((code_rows, HEAD_SIZE), lambda i: (0, 2)),
            whole(column_scale_quantized),
            whole(second_row),
            whole(down_rows),
        ],
        out_specs=vmem(4),
        out_shape=[
            sds((row_count, width), BF16),
            sds((row_count, rank), BF16),
            sds((NIBBLES, half, row_count), F32),
            sds((NIBBLES, half, row_count), BF16),
        ],
        scratch_shapes=project_scratch + [pltpu.VMEM((HEAD_SIZE, row_count), F32)],
        cost_estimate=project_cost,
        name="key_value_projection",
    )(
        layer_input,
        gain_row,
        codes,
        codes,
        column_scale_quantized,
        second_row,
        down_rows,
    )
    kv_got = swap(kv_send)

    def query_projection(first, dtype):
        return pl.pallas_call(
            functools.partial(query_kernel, first),
            in_specs=vmem(4),
            out_specs=pl.BlockSpec(memory_space=pltpu.VMEM),
            out_shape=sds((NIBBLES, HEAD_SIZE, row_count), dtype),
            scratch_shapes=project_scratch,
            cost_estimate=project_cost,
            name="query_send" if first else "query_own",
        )(normed, codes, column_scale_quantized, second_row)

    q_send = query_projection(True, BF16)
    block, cosine, sine = pl.pallas_call(
        key_value_finish_kernel,
        in_specs=vmem(3),
        out_specs=vmem(3),
        out_shape=[
            sds((1, 4 * row_count + GROUP, HEAD_SIZE), BF16),
            sds((half, row_count), F32),
            sds((half, row_count), F32),
        ],
        cost_estimate=cost(1e9, 1e6),
        name="key_value_finish",
    )(kv_own, kv_got, ids_row)
    q_got = swap(q_send)
    q_own = query_projection(False, F32)
    queries = pl.pallas_call(
        query_finish_kernel,
        in_specs=vmem(6),
        out_specs=pl.BlockSpec(memory_space=pltpu.VMEM),
        out_shape=sds((heads, row_count, HEAD_SIZE), BF16),
        scratch_shapes=[pltpu.VMEM((NIBBLES, HEAD_SIZE, row_count), F32)],
        cost_estimate=cost(2e9, 1e6),
        name="query_finish",
    )(q_own, q_got, low_rank, query_up_map, cosine, sine)

    bit = context // 2
    while bit > 2:
        block = jnp.concatenate([block, flip(block, bit)], axis=0)
        bit //= 2
    beside = flip(block, 2)
    core = flip(block, 1)
    core_beside = flip(beside, 1)

    total = width // 2 + query_width // 2
    stacked = (2, heads // 2 * row_count, HEAD_SIZE)
    doubled = (2, heads // 2 * row_count, 2 * HEAD_SIZE)
    attn, mine, other = pl.pallas_call(
        functools.partial(attention_kernel, context),
        in_specs=vmem(11),
        out_specs=vmem(3),
        out_shape=[
            sds((row_count, query_width), BF16),
            sds((rank, total), F32),
            sds((rank, total), BF16),
        ],
        scratch_shapes=[
            pltpu.VMEM(stacked, BF16),
            pltpu.VMEM(stacked, F32),
            pltpu.VMEM(stacked, F32),
            pltpu.VMEM(stacked, F32),
            pltpu.VMEM(doubled, F32),
            pltpu.VMEM(stacked, F32),
            pltpu.VMEM((row_count, query_width), BF16),
        ],
        cost_estimate=cost(1e10, 1e6),
        name="attention",
    )(
        queries,
        output_cotangent,
        block,
        beside,
        core,
        core_beside,
        low_rank,
        normed,
        query_up_map,
        cosine,
        sine,
    )

    summed = mine + flip(other, 1).astype(F32)
    bit = 2
    while bit < context:
        summed = summed + flip(summed.astype(BF16), bit).astype(F32)
        bit *= 2
    down = summed[:, : width // 2]
    down = down + swap(down.astype(BF16)).astype(F32)
    packed = jnp.concatenate([down, summed[:, width // 2 :]], axis=1)
    partner = flip(packed, 1)
    low = (lax.axis_index("ctx") & 1) == 0
    first = jnp.where(low, packed, partner)
    second = jnp.where(low, partner, packed)
    grad_a = jnp.concatenate([first[:, : width // 2], second[:, : width // 2]], axis=1).T
    up_map_gradient = jnp.concatenate([first[:, width // 2 :], second[:, width // 2 :]], axis=1)
    return (attn, grad_a, up_map_gradient)


def solution(mesh):
    return jax.shard_map(
        functools.partial(on_device, mesh.shape["ctx"]),
        mesh=mesh,
        in_specs=(
            P("ctx", None),
            P(),
            P("fsdp", None),
            P("fsdp", None),
            P(),
            P(),
            P(None, "fsdp"),
            P("ctx"),
            P("ctx", "fsdp"),
        ),
        out_specs=(P("ctx", "fsdp"), P(), P(None, "fsdp")),
        check_vma=False,
    )
```

```python
import functools
import math

import jax
import jax.numpy as jnp
from jax import lax
from jax.experimental import pallas as pl
from jax.experimental.pallas import tpu as pltpu
from jax.sharding import PartitionSpec as P

HEAD_SIZE = 128
BLOCK_ROWS = 64
NIBBLES = 8
GROUP = HEAD_SIZE // NIBBLES
DEPTH = 256
STRIP = 16
TOP_BITS = [8 << (4 * n) for n in range(7)] + [-(1 << 31)]

NF4_LEVELS = [
    -1.0,
    -0.6961928009986877,
    -0.5250730514526367,
    -0.39491748809814453,
    -0.28444138169288635,
    -0.18477343022823334,
    -0.09105003625154495,
    0.0,
    0.07958029955625534,
    0.16093020141124725,
    0.24611230194568634,
    0.33791524171829224,
    0.44070982933044434,
    0.5626170039176941,
    0.7229568362236023,
    1.0,
]
LIMIT = pltpu.CompilerParams(vmem_limit_bytes=16 * 2**20)
WIDE_LIMIT = pltpu.CompilerParams(vmem_limit_bytes=40 * 2**20)
ADAPTER_SCALE = 2.0
ROPE_BASE = 500000.0
F32 = jnp.float32
BF16 = jnp.bfloat16


def vmem(count):
    return [pl.BlockSpec(memory_space=pltpu.VMEM)] * count


def nt(a, b):
    return lax.dot_general(a, b, (((1,), (1,)), ((), ())), preferred_element_type=F32)


def tn(a, b):
    return lax.dot_general(a, b, (((0,), (0,)), ((), ())), preferred_element_type=F32)


def nn(a, b):
    return jnp.dot(a, b, preferred_element_type=F32)


def feature_permutation():
    place = lax.broadcasted_iota(jnp.int32, (HEAD_SIZE, HEAD_SIZE), 0)
    feature = lax.broadcasted_iota(jnp.int32, (HEAD_SIZE, HEAD_SIZE), 1)
    hit = feature == NIBBLES * (place % GROUP) + place // GROUP
    return jnp.where(hit, 1.0, 0.0).astype(BF16)


def spread_scales(scale_ref, second_ref, member, sub_tiles, out_ref):
    blocks = scale_ref.shape[0]
    width = second_ref.shape[1]
    row = lax.broadcasted_iota(jnp.int32, (blocks, width), 0) + member * blocks
    lane = lax.broadcasted_iota(jnp.int32, (blocks, width), 1)
    second = jnp.sum(jnp.where(row == lane, second_ref[...], 0.0), axis=1, keepdims=True)
    order = feature_permutation()
    turned = []
    for tile in sub_tiles:
        if isinstance(tile, int):
            codes = scale_ref[:, tile * HEAD_SIZE : (tile + 1) * HEAD_SIZE]
        else:
            codes = scale_ref[:, pl.ds(pl.multiple_of(tile * HEAD_SIZE, HEAD_SIZE), HEAD_SIZE)]
        absmax = (codes.astype(F32) + 1.0) / 256.0 * second
        turned.append(nt(order, absmax.astype(BF16)))
    for n in range(NIBBLES):
        column = jnp.concatenate([t[n * GROUP : (n + 1) * GROUP] for t in turned], axis=0)
        out_ref[n] = column.T


def code_words_copies(codes_ref, lane_start, buffer_ref, sems_ref):
    steps = buffer_ref.shape[0]
    return [
        pltpu.make_async_copy(
            codes_ref.at[pl.ds(step * DEPTH, DEPTH), pl.ds(lane_start, 2 * HEAD_SIZE)],
            buffer_ref.at[step],
            sems_ref.at[step],
        )
        for step in range(steps)
    ]


def pick(table, index):
    numbers = lax.GatherDimensionNumbers(
        offset_dims=(),
        collapsed_slice_dims=(0,),
        start_index_map=(0,),
        operand_batching_dims=(1,),
        start_indices_batching_dims=(1,),
    )
    mode = lax.GatherScatterMode.PROMISE_IN_BOUNDS
    return lax.gather(table, index[..., None], numbers, slice_sizes=(1, 1), mode=mode)


def table_rows(levels):
    place = lax.broadcasted_iota(jnp.int32, (8, HEAD_SIZE), 0)
    table = jnp.zeros((8, HEAD_SIZE), F32)
    for index, level in enumerate(levels):
        table = jnp.where(place == index, F32(level), table)
    return table


def project(words, wait, x_ref, x_start, scales_ref, weight_ref, total_ref, row_count):
    steps = row_count // DEPTH
    tables = (table_rows(NF4_LEVELS[:8]), table_rows(NF4_LEVELS[8:]))

    def fill(step, slot):
        wait(step)
        for part in range(DEPTH // BLOCK_ROWS):
            word = words(step, part)
            block = step * (DEPTH // BLOCK_ROWS) + part
            rows = slice(part * BLOCK_ROWS, (part + 1) * BLOCK_ROWS)
            for n in range(NIBBLES):
                scale = scales_ref[n, pl.ds(block, 1), :]
                index = (lax.shift_right_logical(word, 4 * n) if n else word) & 7
                upper = (word & jnp.int32(TOP_BITS[n])) != 0
                pieces = []
                for k in range(0, BLOCK_ROWS, 8):
                    low, high = (pick(table, index[k : k + 8]) for table in tables)
                    pieces.append(jnp.where(upper[k : k + 8], high, low) * scale)
                weight = jnp.concatenate(pieces, axis=0).astype(BF16)
                weight_ref[slot, n, rows, :] = weight

    def multiply(step, slot):
        start = pl.multiple_of(x_start + step * DEPTH, DEPTH)
        left = x_ref[:, pl.ds(start, DEPTH)]
        for pair in range(NIBBLES // 2):
            right = jnp.concatenate(
                [weight_ref[slot, 2 * pair], weight_ref[slot, 2 * pair + 1]], axis=1
            )
            columns = slice(2 * pair * HEAD_SIZE, 2 * (pair + 1) * HEAD_SIZE)
            total_ref[:, columns] += nn(left, right)

    total_ref[...] = jnp.zeros_like(total_ref)
    fill(0, 0)

    def body(step, carry):
        multiply(step - 1, (step - 1) % 2)
        fill(step, step % 2)
        return carry

    lax.fori_loop(1, steps, body, 0)
    multiply(steps - 1, (steps - 1) % 2)


def key_value_kernel(
    x_ref,
    gain_ref,
    codes_ref,
    scale_ref,
    second_ref,
    normed_ref,
    own_ref,
    send_ref,
    scales_ref,
    weight_ref,
    total_ref,
    turned_ref,
    words_ref,
    sems_ref,
):
    member = lax.axis_index("fsdp")
    row_count = codes_ref.shape[0]
    copies = code_words_copies(codes_ref, HEAD_SIZE, words_ref, sems_ref)
    for copy in copies:
        copy.start()
    wide = x_ref[...].astype(F32)
    inverse = lax.rsqrt(jnp.mean(wide * wide, axis=-1, keepdims=True) + 1e-05)
    normed_ref[...] = (wide * inverse * gain_ref[...]).astype(BF16)
    spread_scales(scale_ref, second_ref, member, [8, 9, 10, 11, 20, 21, 22, 23], scales_ref)
    lane = lax.broadcasted_iota(jnp.int32, (BLOCK_ROWS, HEAD_SIZE), 1)

    def words(step, part):
        rows = slice(part * BLOCK_ROWS, (part + 1) * BLOCK_ROWS)
        low = words_ref[step, rows, :HEAD_SIZE]
        high = words_ref[step, rows, HEAD_SIZE:]
        return jnp.where(lane < HEAD_SIZE // 2, low, high)

    def wait(step):
        pltpu.make_async_copy(
            codes_ref.at[pl.ds(0, DEPTH), pl.ds(HEAD_SIZE, 2 * HEAD_SIZE)],
            words_ref.at[step],
            sems_ref.at[step],
        ).wait()

    project(
        words, wait, normed_ref, member * row_count, scales_ref, weight_ref, total_ref, row_count
    )
    half = HEAD_SIZE // 2
    for n in range(NIBBLES):
        turned_ref[...] = total_ref[:, n * HEAD_SIZE : (n + 1) * HEAD_SIZE].T
        own_ref[n] = turned_ref[pl.ds(pl.multiple_of(member * half, half), half), :]
        other = turned_ref[pl.ds(pl.multiple_of((1 - member) * half, half), half), :]
        send_ref[n] = other.astype(BF16)


def query_kernel(
    first,
    normed_hbm_ref,
    codes_ref,
    scale_ref,
    second_ref,
    out_ref,
    scales_ref,
    weight_ref,
    total_ref,
    words_ref,
    sems_ref,
    x_ref,
    x_sem,
):
    member = lax.axis_index("fsdp")
    target = (1 - member) if first else member
    row_count = codes_ref.shape[0]
    lane_start = pl.multiple_of(target * HEAD_SIZE, HEAD_SIZE)
    fetch = pltpu.make_async_copy(
        normed_hbm_ref.at[:, pl.ds(pl.multiple_of(member * row_count, HEAD_SIZE), row_count)],
        x_ref,
        x_sem,
    )
    copies = code_words_copies(codes_ref, lane_start, words_ref, sems_ref)
    copies[0].start()
    fetch.start()
    for copy in copies[1:]:
        copy.start()
    tiles = [
        jnp.where(target == 0, k, (16 + k) if k < 4 else (8 + k)) for k in range(NIBBLES)
    ]
    spread_scales(scale_ref, second_ref, member, tiles, scales_ref)
    lane = lax.broadcasted_iota(jnp.int32, (BLOCK_ROWS, HEAD_SIZE), 1)
    take_high = (lane < HEAD_SIZE // 2) & (target == 1)

    def words(step, part):
        rows = slice(part * BLOCK_ROWS, (part + 1) * BLOCK_ROWS)
        low = words_ref[step, rows, :HEAD_SIZE]
        high = words_ref[step, rows, HEAD_SIZE:]
        return jnp.where(take_high, high, low)

    def wait(step):
        pltpu.make_async_copy(
            codes_ref.at[pl.ds(0, DEPTH), pl.ds(0, 2 * HEAD_SIZE)],
            words_ref.at[step],
            sems_ref.at[step],
        ).wait()

    fetch.wait()
    project(words, wait, x_ref, 0, scales_ref, weight_ref, total_ref, row_count)
    for n in range(NIBBLES):
        out_ref[n] = total_ref[:, n * HEAD_SIZE : (n + 1) * HEAD_SIZE].T.astype(out_ref.dtype)


def rotate_pair(a, b, cosine, sine):
    return a * cosine - b * sine, b * cosine + a * sine


def key_value_finish_kernel(own_ref, got_ref, ids_ref, block_ref, cosine_ref, sine_ref):
    row_count = own_ref.shape[2]
    place = lax.axis_index("ctx")
    half = HEAD_SIZE // 2
    row = lax.broadcasted_iota(jnp.int32, (half, row_count), 0)
    token = lax.broadcasted_iota(jnp.int32, (half, row_count), 1) + place * row_count
    index = NIBBLES * (row % NIBBLES) + row // NIBBLES
    freqs = jnp.exp(index.astype(F32) * (-2.0 * math.log(ROPE_BASE) / HEAD_SIZE))
    angle = token.astype(F32) * freqs
    cosine_ref[...] = jnp.cos(angle)
    sine_ref[...] = jnp.sin(angle)
    order = feature_permutation()
    full = [own_ref[n] + got_ref[n].astype(F32) for n in range(NIBBLES)]
    for head in range(2):
        pieces = []
        for n in range(NIBBLES):
            group = full[n][head * GROUP : (head + 1) * GROUP]
            rows = slice(n * NIBBLES, (n + 1) * NIBBLES)
            pieces.extend(
                rotate_pair(group[:NIBBLES], group[NIBBLES:], cosine_ref[rows], sine_ref[rows])
            )
        keys = jnp.concatenate(pieces, axis=0).T.astype(BF16)
        block_ref[0, head * row_count : (head + 1) * row_count, :] = keys
        values = jnp.concatenate(
            [full[n][(2 + head) * GROUP : (3 + head) * GROUP] for n in range(NIBBLES)], axis=0
        )
        values = nn(values.T.astype(BF16), order).astype(BF16)
        block_ref[0, (2 + head) * row_count : (3 + head) * row_count, :] = values
    ids = jnp.broadcast_to(ids_ref[...].astype(F32), (GROUP, row_count))
    block_ref[0, 4 * row_count :, :] = ids.astype(BF16)


def query_finish_kernel(
    own_ref,
    got_ref,
    normed_ref,
    down_ref,
    up_ref,
    cosine_ref,
    sine_ref,
    queries_ref,
    low_rank_ref,
    full_ref,
):
    member = lax.axis_index("fsdp")
    low_rank_ref[...] = nt(normed_ref[...], down_ref[...]).astype(BF16)
    order = feature_permutation()
    heads = queries_ref.shape[0]
    for n in range(NIBBLES):
        full_ref[n] = own_ref[n] + got_ref[n].astype(F32)
    for head in range(heads):
        up = nt(up_ref[:, head * HEAD_SIZE : (head + 1) * HEAD_SIZE], order).astype(BF16)
        adapter = ADAPTER_SCALE * lax.dot_general(
            up, low_rank_ref[...], (((0,), (1,)), ((), ())), preferred_element_type=F32
        )
        start = pl.multiple_of(((head + member * (heads // 2)) % heads) * GROUP, GROUP)
        pieces = []
        for n in range(NIBBLES):
            group = full_ref[n, pl.ds(start, GROUP), :] + adapter[n * GROUP : (n + 1) * GROUP]
            rows = slice(n * NIBBLES, (n + 1) * NIBBLES)
            pieces.extend(
                rotate_pair(group[:NIBBLES], group[NIBBLES:], cosine_ref[rows], sine_ref[rows])
            )
        queries_ref[head] = jnp.concatenate(pieces, axis=0).T.astype(BF16)


def attention_kernel(context, flips, first, *refs):
    queries_ref, cotangent_ref = refs[:2]
    pieces = refs[2:4]
    if first:
        ids_ref = pieces[0]
        state = refs[4:9]
        before = None
        bias_ref, scores_ref, dots_ref, expo_ref = refs[9:13]
    else:
        ids_ref = refs[4]
        before = refs[5:10]
        low_rank_ref, normed_ref, up_ref, cosine_ref, sine_ref = refs[10:15]
        attn_ref, mine_ref, other_ref = refs[15:18]
        state = refs[18:23]
        bias_ref, scores_ref, dots_ref, expo_ref, lin_ref = refs[23:28]
    top_ref, norm_ref, dot_ref, out_ref, grad_ref = state
    place = lax.axis_index("ctx")
    heads, row_count, _ = queries_ref.shape
    grouped = heads // 2
    stack = grouped * row_count
    lists = pieces[0].shape[0]
    taken = min(lists, 4)
    span = taken * len(pieces) * row_count
    depth = context.bit_length() - 1
    soft = math.log2(math.e) / math.sqrt(HEAD_SIZE)
    square = (row_count, row_count)
    my_ids = ids_ref[0, 4 * row_count :, :].astype(F32)[:1]
    row_ids = jnp.broadcast_to(my_ids, square).T
    row_pos = lax.broadcasted_iota(jnp.int32, square, 0) + place * row_count
    lane = lax.broadcasted_iota(jnp.int32, square, 1)

    def device_of(number):
        flip = 0
        for b in range(depth - 2):
            flip = flip + (((number >> b) & 1) << (depth - 1 - b))
        return place ^ flip

    def lowest(step):
        highest = depth - 3 - (taken.bit_length() - 1)
        kept = device_of(step * taken) & ~(context - 1 - ((1 << (highest + 3)) - 1))
        return kept & ~3

    def chunk(start, source):
        numbers = [start + k for k in range(taken)]
        blocks = [(piece, number) for piece in pieces for number in numbers]
        for index, (piece, number) in enumerate(blocks):
            device = device_of(number) ^ flips[index // taken]
            ids = piece[number, 4 * row_count :, :].astype(F32)[:1]
            pos = lane + device * row_count
            allowed = (row_ids == ids) & (pos <= row_pos)
            bias_ref[:, index * row_count : (index + 1) * row_count] = jnp.where(
                allowed, 0.0, -1e30
            )
        for kv in range(2):
            key_rows = slice(kv * row_count, (kv + 1) * row_count)
            value_rows = slice((2 + kv) * row_count, (3 + kv) * row_count)
            keys = jnp.concatenate([p[k, key_rows, :] for p, k in blocks], axis=0)
            values = jnp.concatenate([p[k, value_rows, :] for p, k in blocks], axis=0)
            query = queries_ref[kv * grouped : (kv + 1) * grouped].reshape(stack, HEAD_SIZE)
            grads = jnp.concatenate(
                [
                    cotangent_ref[:, (kv * grouped + g) * HEAD_SIZE : (kv * grouped + g + 1) * HEAD_SIZE]
                    for g in range(grouped)
                ],
                axis=0,
            )
            scores_ref[kv] = nt(query, keys)
            dots_ref[kv] = nt(grads, values)
        for kv in range(2):
            key_rows = slice(kv * row_count, (kv + 1) * row_count)
            value_rows = slice((2 + kv) * row_count, (3 + kv) * row_count)
            decays = []
            for strip in range(stack // STRIP):
                rows = slice(strip * STRIP, (strip + 1) * STRIP)
                at = strip * STRIP % row_count
                scores = scores_ref[kv, rows, :] * soft + bias_ref[at : at + STRIP, :]
                new = jnp.max(scores, axis=1, keepdims=True)
                if source is not None:
                    old = source[0][kv, rows, :]
                    new = jnp.maximum(old, new)
                    decay = jnp.exp2(old - new)
                    decays.append(decay)
                else:
                    new = jnp.broadcast_to(new, (STRIP, HEAD_SIZE))
                wide = jnp.concatenate([new] * (span // HEAD_SIZE), axis=1)
                expo = jnp.exp2(scores - wide)
                weighted = expo * dots_ref[kv, rows, :]
                norm = fold(expo)
                dot = fold(weighted)
                if source is not None:
                    norm = norm + decay * source[1][kv, rows, :]
                    dot = dot + decay * source[2][kv, rows, :]
                top_ref[kv, rows, :] = new
                norm_ref[kv, rows, :] = norm
                dot_ref[kv, rows, :] = dot
                expo_ref[kv, rows, :] = expo.astype(BF16)
                expo_ref[kv, stack + strip * STRIP : stack + (strip + 1) * STRIP, :] = (
                    weighted.astype(BF16)
                )
            both = jnp.concatenate(
                [
                    jnp.concatenate([p[k, value_rows, :], p[k, key_rows, :]], axis=1)
                    for p, k in blocks
                ],
                axis=0,
            )
            product = nn(expo_ref[kv, :stack, :], both)
            graded = nn(expo_ref[kv, stack:, :], both[:, HEAD_SIZE:])
            if source is not None:
                decay = jnp.concatenate(decays, axis=0)
                product = product + jnp.concatenate([decay, decay], axis=1) * source[3][kv]
                graded = graded + decay * source[4][kv]
            out_ref[kv] = product
            grad_ref[kv] = graded

    chunk(0, before)
    if lists > taken:

        def body(step, carry):

            @pl.when(lowest(step) <= place)
            def _():
                chunk(step * taken, state)

            return carry

        lax.fori_loop(1, lists // taken, body, 0)
    if first:
        return

    cosine, sine = [], []
    for n in range(NIBBLES):
        rows = slice(n * NIBBLES, (n + 1) * NIBBLES)
        cosine.extend([cosine_ref[rows]] * 2)
        sine.extend([sine_ref[rows], -sine_ref[rows]])
    cosine = jnp.concatenate(cosine, axis=0).T
    sine = jnp.concatenate(sine, axis=0).T
    low_half = (lax.broadcasted_iota(jnp.int32, square, 1) & NIBBLES) == 0
    order = feature_permutation()
    for head in range(heads):
        kv, g = divmod(head, grouped)
        rows = slice(g * row_count, (g + 1) * row_count)
        columns = slice(head * HEAD_SIZE, (head + 1) * HEAD_SIZE)
        inverse = 1.0 / jnp.sum(norm_ref[kv, rows, :], axis=1, keepdims=True)
        attn_ref[:, columns] = (out_ref[kv, rows, :HEAD_SIZE] * inverse).astype(BF16)
        mean = jnp.sum(dot_ref[kv, rows, :], axis=1, keepdims=True) * inverse
        grad = (grad_ref[kv, rows, :] - mean * out_ref[kv, rows, HEAD_SIZE:]) * (
            inverse * (1.0 / math.sqrt(HEAD_SIZE))
        )
        swapped = jnp.where(
            low_half,
            pltpu.roll(grad, HEAD_SIZE - NIBBLES, 1),
            pltpu.roll(grad, NIBBLES, 1),
        )
        lin = (grad * cosine + swapped * sine).astype(BF16)
        lin_ref[:, columns] = nn(lin, order).astype(BF16)
    middle = (ADAPTER_SCALE * nt(lin_ref[...], up_ref[...])).astype(BF16)
    core = place & 1
    width = normed_ref.shape[1] // 2
    up_width = lin_ref.shape[1] // 2
    mine = pl.ds(pl.multiple_of(core * width, HEAD_SIZE), width)
    other = pl.ds(pl.multiple_of((1 - core) * width, HEAD_SIZE), width)
    mine_ref[:, :width] = tn(middle, normed_ref[:, mine])
    other_ref[:, :width] = tn(middle, normed_ref[:, other]).astype(BF16)
    mine = pl.ds(pl.multiple_of(core * up_width, HEAD_SIZE), up_width)
    other = pl.ds(pl.multiple_of((1 - core) * up_width, HEAD_SIZE), up_width)
    mine_ref[:, width:] = ADAPTER_SCALE * tn(low_rank_ref[...], lin_ref[:, mine])
    other_ref[:, width:] = (ADAPTER_SCALE * tn(low_rank_ref[...], lin_ref[:, other])).astype(BF16)


def fold(a):
    total = a[:, :HEAD_SIZE]
    for start in range(HEAD_SIZE, a.shape[1], HEAD_SIZE):
        total = total + a[:, start : start + HEAD_SIZE]
    return total


def cost(flops, size):
    return pl.CostEstimate(flops=int(flops), bytes_accessed=int(size), transcendentals=0)


def on_device(
    context,
    layer_input,
    gain,
    codes,
    column_scale_quantized,
    block_second_scale,
    query_down_map,
    query_up_map,
    token_document,
    output_cotangent,
):
    row_count, width = layer_input.shape
    code_rows, code_width = codes.shape
    rank = query_down_map.shape[1]
    query_width = query_up_map.shape[1]
    heads = query_width // HEAD_SIZE
    half = HEAD_SIZE // 2
    sds = jax.ShapeDtypeStruct

    def flip(array, bit):
        return lax.ppermute(array, "ctx", [(i, i ^ bit) for i in range(context)])

    def swap(array):
        return lax.ppermute(array, "fsdp", [(0, 1), (1, 0)])

    gain_row = gain.reshape(1, width)
    second_row = block_second_scale.reshape(1, -1)
    ids_row = token_document.reshape(1, row_count)
    down_rows = query_down_map.T
    steps = code_rows // DEPTH
    project_scratch = [
        pltpu.VMEM((NIBBLES, code_rows // BLOCK_ROWS, HEAD_SIZE), F32),
        pltpu.VMEM((2, NIBBLES, DEPTH, HEAD_SIZE), BF16),
        pltpu.VMEM((row_count, NIBBLES * HEAD_SIZE), F32),
    ]
    words_scratch = [
        pltpu.VMEM((steps, DEPTH, 2 * HEAD_SIZE), jnp.int32),
        pltpu.SemaphoreType.DMA((steps,)),
    ]
    project_cost = cost(1.2e10, code_rows * HEAD_SIZE * 4)
    anywhere = pl.BlockSpec(memory_space=pl.ANY)
    normed, kv_own, kv_send = pl.pallas_call(
        key_value_kernel,
        in_specs=vmem(2) + [anywhere] + vmem(2),
        out_specs=vmem(3),
        out_shape=[
            sds((row_count, width), BF16),
            sds((NIBBLES, half, row_count), F32),
            sds((NIBBLES, half, row_count), BF16),
        ],
        scratch_shapes=project_scratch + [pltpu.VMEM((HEAD_SIZE, row_count), F32)] + words_scratch,
        cost_estimate=project_cost,
        compiler_params=LIMIT,
        name="key_value_projection",
    )(layer_input, gain_row, codes, column_scale_quantized, second_row)
    kv_got = swap(kv_send)

    def query_projection(first, dtype):
        return pl.pallas_call(
            functools.partial(query_kernel, first),
            in_specs=[anywhere] * 2 + vmem(2),
            out_specs=pl.BlockSpec(memory_space=pltpu.VMEM),
            out_shape=sds((NIBBLES, HEAD_SIZE, row_count), dtype),
            scratch_shapes=project_scratch
            + words_scratch
            + [pltpu.VMEM((row_count, code_rows), BF16), pltpu.SemaphoreType.DMA],
            cost_estimate=project_cost,
            compiler_params=LIMIT,
        name="query_send" if first else "query_own",
        )(normed, codes, column_scale_quantized, second_row)

    q_send = query_projection(True, BF16)
    q_got = swap(q_send)
    kv_got, q_send = lax.optimization_barrier((kv_got, q_send))
    block, cosine, sine = pl.pallas_call(
        key_value_finish_kernel,
        in_specs=vmem(3),
        out_specs=vmem(3),
        out_shape=[
            sds((1, 4 * row_count + GROUP, HEAD_SIZE), BF16),
            sds((half, row_count), F32),
            sds((half, row_count), F32),
        ],
        cost_estimate=cost(1e9, 1e6),
        compiler_params=LIMIT,
        name="key_value_finish",
    )(kv_own, kv_got, ids_row)
    q_own = query_projection(False, F32)
    queries, low_rank = pl.pallas_call(
        query_finish_kernel,
        in_specs=vmem(7),
        out_specs=vmem(2),
        out_shape=[sds((heads, row_count, HEAD_SIZE), BF16), sds((row_count, rank), BF16)],
        scratch_shapes=[pltpu.VMEM((NIBBLES, HEAD_SIZE, row_count), F32)],
        cost_estimate=cost(2e9, 1e6),
        compiler_params=LIMIT,
        name="query_finish",
    )(q_own, q_got, normed, down_rows, query_up_map, cosine, sine)

    bit = context // 2
    beside_work = [q_own, queries]
    while bit > 2:
        got = flip(block, bit)
        if beside_work:
            got, _ = lax.optimization_barrier((got, beside_work.pop(0)))
        block = jnp.concatenate([block, got], axis=0)
        bit //= 2
    beside = flip(block, 2)
    core = flip(block, 1)

    lists = block.shape[0]
    span = min(lists, 4) * 2 * row_count
    stack = heads // 2 * row_count
    state_shapes = [(2, stack, HEAD_SIZE)] * 3 + [(2, stack, 2 * HEAD_SIZE), (2, stack, HEAD_SIZE)]
    work_shapes = [
        pltpu.VMEM((row_count, span), F32),
        pltpu.VMEM((2, stack, span), F32),
        pltpu.VMEM((2, stack, span), F32),
        pltpu.VMEM((2, 2 * stack, span), BF16),
    ]
    state = pl.pallas_call(
        functools.partial(attention_kernel, context, (0, 1), True),
        in_specs=vmem(4),
        out_specs=vmem(5),
        out_shape=[sds(shape, F32) for shape in state_shapes],
        scratch_shapes=work_shapes,
        cost_estimate=cost(8e9, 1e6),
        compiler_params=WIDE_LIMIT,
        name="attention_near",
    )(queries, output_cotangent, block, core)
    beside, state = lax.optimization_barrier((beside, tuple(state)))
    core_beside = flip(beside, 1)
    total = width // 2 + query_width // 2
    attn, mine, other = pl.pallas_call(
        functools.partial(attention_kernel, context, (2, 3), False),
        in_specs=vmem(15),
        out_specs=vmem(3),
        out_shape=[
            sds((row_count, query_width), BF16),
            sds((rank, total), F32),
            sds((rank, total), BF16),
        ],
        scratch_shapes=[pltpu.VMEM(shape, F32) for shape in state_shapes]
        + work_shapes
        + [pltpu.VMEM((row_count, query_width), BF16)],
        cost_estimate=cost(1e10, 1e6),
        compiler_params=WIDE_LIMIT,
        name="attention_far",
    )(
        queries,
        output_cotangent,
        beside,
        core_beside,
        block,
        *state,
        low_rank,
        normed,
        query_up_map,
        cosine,
        sine,
    )

    summed = mine + flip(other, 1).astype(F32)
    bit = 2
    while bit < context:
        summed = summed + flip(summed.astype(BF16), bit).astype(F32)
        bit *= 2
    down = summed[:, : width // 2]
    down = down + swap(down.astype(BF16)).astype(F32)
    packed = jnp.concatenate([down, summed[:, width // 2 :]], axis=1)
    partner = flip(packed, 1)
    low = (lax.axis_index("ctx") & 1) == 0
    first = jnp.where(low, packed, partner)
    second = jnp.where(low, partner, packed)
    grad_a = jnp.concatenate([first[:, : width // 2], second[:, : width // 2]], axis=1).T
    up_map_gradient = jnp.concatenate([first[:, width // 2 :], second[:, width // 2 :]], axis=1)
    return (attn, grad_a, up_map_gradient)


def solution(mesh):
    return jax.shard_map(
        functools.partial(on_device, mesh.shape["ctx"]),
        mesh=mesh,
        in_specs=(
            P("ctx", None),
            P(),
            P("fsdp", None),
            P("fsdp", None),
            P(),
            P(),
            P(None, "fsdp"),
            P("ctx"),
            P("ctx", "fsdp"),
        ),
        out_specs=(P("ctx", "fsdp"), P(), P(None, "fsdp")),
        check_vma=False,
    )
```
